32 devices in a mesh: gx: 2 (over y), gy: 4 (over z), gz: 4 (over x, core).
Axes of the slice: x: 2, y: 2, z: 4, core: 2. Of those that a mesh axis runs over, the one named last changes fastest.
Arguments:
- eri: bfloat16 [1024, 256, 256], P(('gx', 'gy', 'gz')), may hold values from -0.375 to 0.375
- owner: int32 [1024, 1], P(('gx', 'gy', 'gz')), may hold values from 0 to 1; in each aligned block of 32 rows (0 to 31, 32 to 63, ...) at most 32 rows name the same one
- quartet: int32 [1024, 4], P(('gx', 'gy', 'gz')), may hold values from 0 to 191, as said below
- significance: int32 [1024], P(('gx', 'gy', 'gz')), may hold values 0 or 1
- density: bfloat16 [3072, 3072], P('gy'), may hold values from -6 to 6
Outputs:
- exchange: float32 [3072, 3072], P('gx', 'gy')
The draws below stay inside these ranges and needn't reach their ends.
Inputs may be any that keep to these rules, and one draw needn't show every extreme that they name: Among the 32 tiles of one device (aligned blocks of 32 rows), no owner value is named more than 32 times, and in some blocks one is named exactly 32 times. `quartet`: column 0 lies in 0 to 23, column 1 in 0 to 191, column 2 in 0 to 47, column 3 in 0 to 191.
All inputs are finite; a program needn't handle non-finite values. No bound on the sum of `significance` on one device may be relied on, other than what follows from the above.
Results may differ from the reference program's by a relative error of at most 0.0003.
Values sent between devices are 32-bit elements; how exact they have to be, the bound alone decides.
A program may use at most 128 MiB of HBM per device.

```python
import math
import jax
import jax.numpy as jnp
import numpy as np
from jax import lax

NBAS = 3072
SHELL = 16
TILES_DEV = 32
NSH = 192
ROWSH = 24
DSLAB = 48
CAP = 32
TILES = 1024
N_GX = 2
N_GY = 4
N_GZ = 4


def draw_quartet(key, part):
    upper = jnp.array([ROWSH, NSH, DSLAB, NSH], dtype=jnp.int32)
    return jax.random.randint(key, (TILES, 4), 0, upper, dtype=jnp.int32)


def touch_ends(values, key, least, largest):
    dims = values.shape
    spot = [jax.random.randint(jax.random.fold_in(key, axis), (), 0, dims[axis]) for axis in range(len(dims))]
    values = values.at[tuple(spot)].set(least)
    longest = dims.index(max(dims))
    spot[longest] = (spot[longest] + 1) % dims[longest]
    return values.at[tuple(spot)].set(largest)


def level_of(key, extent, split, low, high):
    factor_of, own = 1.0, jax.random.fold_in(key, 6)
    for dim, parts in split:
        heights = jnp.exp(jax.random.uniform(jax.random.fold_in(own, dim), (parts,), jnp.float32, low / len(split), high / len(split)))
        factor_of = factor_of * jnp.repeat(heights, extent[dim] // parts).reshape([-1 if axis == dim else 1 for axis in range(len(extent))])
    return factor_of


def assign_block(rng, own, number, rows, count, top, limit, slope):
    order = jax.random.permutation(rng, count)
    crowded, ordinary = portions_of(count, rows * top, limit, slope, True), portions_of(count, rows * top, limit, slope, False)
    places = jnp.arange(count)

    def named(lengths, turn):
        used = int((lengths > 0).sum())
        fixed = max(1, used // 4)
        moved = fixed + (places - fixed + turn * (used - fixed)) % max(1, count - fixed)
        return jnp.zeros((count,), jnp.int32).at[order[jnp.where(places < fixed, places, moved)]].set(jnp.asarray(lengths, jnp.int32))

    lengths = jnp.where(number % 4 == 0, named(crowded, number // 4), named(ordinary, number - number // 4 - 1))
    mixed = jax.random.permutation(jax.random.fold_in(own, 3), count)
    donor, sink = mixed[0:count // 2 * 2:2], mixed[1:count // 2 * 2:2]
    room = jnp.minimum(lengths[donor] - 1, limit - lengths[sink]) // 2
    room = jnp.where((donor == order[0]) | (sink == order[0]) | (lengths[sink] == 0), 0, jnp.maximum(room, 0))
    moved = jax.random.randint(jax.random.fold_in(own, 4), (count // 2,), 0, 1 << 20) % (room + 1)
    lengths = lengths.at[donor].add(-moved).at[sink].add(moved)
    labels = jnp.searchsorted(jnp.cumsum(lengths), jnp.arange(rows * top), side="right").astype(jnp.int32)
    table = labels.reshape(top, rows).T
    table = table[jax.random.permutation(jax.random.fold_in(own, 1), rows)]
    turn = jax.random.randint(jax.random.fold_in(own, 2), (rows, 1), 0, top)
    return jnp.take_along_axis(table, (jnp.arange(top)[None, :] + turn) % top, axis=1)


def portions_of(amount, total, bound, slope, full):
    portions = [(1 << 20) // math.isqrt(standing ** slope) + 1 for standing in range(1, amount + 1)]
    largest = bound if full else min(bound, max(-(-total // amount), total * portions[0] // sum(portions)))
    least = 1 if total - largest >= amount - 1 else 0
    holding, surplus = [largest] + [least] * (amount - 1), total - largest - least * (amount - 1)
    while surplus > 0:
        free = [i for i in range(1, amount) if holding[i] < largest] or [i for i in range(1, amount) if holding[i] < bound]
        mass, budget = sum([portions[i] for i in free]), surplus
        for i in free:
            extra = min(bound - holding[i], max(1, budget * portions[i] // mass), surplus)
            holding[i] = holding[i] + extra
            surplus = surplus - extra
    return np.array(holding)


def noise(key, extent, scale, bound, cuts=(), kind=jnp.bfloat16):
    drawn = jax.random.normal(key, extent, jnp.float32) * scale
    if len(cuts) > 0:
        drawn = level_of(key, extent, cuts, -0.22, 0.18) * drawn
    return jnp.clip(drawn, min=-bound, max=bound).astype(kind)


def setup_inputs(seed: int = 0) -> dict:
    seeds = jax.random.split(jax.random.key(seed), 6)
    eri = noise(seeds[0], (TILES, SHELL * SHELL, SHELL * SHELL), (SHELL * SHELL) ** -0.5, 0.375, ((0, 32),))
    owner_keys = jax.random.split(jax.random.fold_in(seeds[1], 1), TILES // TILES_DEV)
    owner_turns = jax.random.permutation(jax.random.fold_in(seeds[1], 3), TILES // TILES_DEV)
    owner = jax.vmap(lambda own, number: assign_block(jax.random.fold_in(seeds[1], 2), own, number, TILES_DEV, N_GX, 1, CAP, 2))(owner_keys, owner_turns).reshape((TILES, 1))
    quartet = draw_quartet(jax.random.fold_in(seeds[5], 71), 0)
    significance = touch_ends((jax.random.randint(seeds[3], (TILES,), 0, 4) < 3).astype(jnp.int32), jax.random.fold_in(seeds[3], 1), 0, 1)
    density = noise(seeds[4], (NBAS, NBAS), 1.0, 6.0, ((0, 4),))
    return dict(eri=eri, owner=owner, quartet=quartet, significance=significance, density=density)


def reference(eri, owner, quartet, significance, density):
    shell_count = NBAS // SHELL
    pair_size = SHELL * SHELL
    density_blocks = density.astype(jnp.float32).reshape(shell_count, SHELL, shell_count, SHELL)
    tile_index = jnp.arange(TILES, dtype=jnp.int32)
    device = tile_index // TILES_DEV
    z_index = device % N_GZ
    y_index = (device // N_GZ) % N_GY
    bra_shell = ((owner[:, 0] * N_GZ + z_index) * ROWSH + quartet[:, 0]).astype(jnp.int32)
    ket_shell = quartet[:, 1].astype(jnp.int32)
    row_shell = (y_index * DSLAB + quartet[:, 2]).astype(jnp.int32)
    col_shell = quartet[:, 3].astype(jnp.int32)
    blocks = density_blocks[row_shell, :, col_shell, :]
    weight = significance.astype(jnp.float32)
    groups = TILES // TILES_DEV

    def contract(operands):
        tile_data, flat_block, tile_weight = operands
        summed = jnp.einsum("tij,tj->ti", tile_data.astype(jnp.float32), flat_block)
        return summed * tile_weight[:, None]

    terms = lax.map(contract, (eri.reshape(groups, TILES_DEV, pair_size, pair_size),
                               blocks.reshape(groups, TILES_DEV, pair_size),
                               weight.reshape(groups, TILES_DEV)))
    terms = terms.reshape(TILES, SHELL, SHELL)
    result = jnp.zeros((shell_count, SHELL, shell_count, SHELL), jnp.float32)
    result = result.at[bra_shell, :, ket_shell, :].add(terms)
    return result.reshape(NBAS, NBAS)
```

```python
import functools

import jax
import jax.numpy as jnp
from jax import lax
from jax.experimental import pallas as pl
from jax.experimental.pallas import tpu as pltpu
from jax.sharding import PartitionSpec as P

SHELL = 16
PACK = 128 // SHELL
MESH = pl.DeviceIdType.MESH


def iota(shape, dim):
    return lax.broadcasted_iota(jnp.int32, shape, dim)


def contract_kernel(ket_bits, row_bits, owner_ref, quartet_ref, keep_ref, eri_ref, density_ref,
                    out_ref, tiles, picked, masked, tile_sem, pick_sem):
    count = eri_ref.shape[0]
    groups = count // PACK
    picks = []
    for t in range(count):
        row = pl.multiple_of(quartet_ref[t, 2] * SHELL, SHELL)
        col = pl.multiple_of((quartet_ref[t, 3] // PACK) * 128, 128)
        pick = pltpu.make_async_copy(density_ref.at[pl.ds(row, SHELL), pl.ds(col, 128)],
                                     picked.at[pl.ds(t * SHELL, SHELL), :], pick_sem.at[t])
        pick.start()
        picks.append(pick)
    loads = []
    for g in range(groups):
        part = pl.ds(g * PACK, PACK)
        load = pltpu.make_async_copy(eri_ref.at[part], tiles.at[part], tile_sem.at[g])
        load.start()
        loads.append(load)

    lane = iota((8, 128), 1)
    codes = jnp.zeros((8, 128), jnp.int32)
    for t in range(count):
        code = (owner_ref[t, 0] << (ket_bits + row_bits)) + (quartet_ref[t, 0] << ket_bits) + quartet_ref[t, 1]
        codes = jnp.where(lane == t, code, codes)
    out_ref[pl.ds(groups * SHELL, 8), :] = codes.astype(jnp.float32)

    block_lane = iota((SHELL, 128), 1) // SHELL
    for t in range(count):
        picks[t].wait()
        place = jnp.where(keep_ref[t] > 0, lax.rem(quartet_ref[t, 3], PACK), -1)
        rows = pl.ds(t * SHELL, SHELL)
        block = picked[rows, :].astype(jnp.float32)
        masked[rows, :] = jnp.where(block_lane == place, block, 0.0).astype(jnp.bfloat16)

    pair = SHELL * SHELL
    repeat = (iota((128, pair), 0) % SHELL == iota((128, pair), 1) % SHELL).astype(jnp.bfloat16)
    own_row = iota((128, pair), 0) % SHELL == iota((128, pair), 1) // SHELL
    same_tile = (iota((128, 128), 0) // SHELL == iota((128, 128), 1) // SHELL).astype(jnp.bfloat16)
    weights = []
    for g in range(groups):
        spread = jnp.dot(masked[pl.ds(g * 128, 128), :], repeat, preferred_element_type=jnp.float32)
        spread = jnp.where(own_row, spread, 0.0).astype(jnp.bfloat16)
        flat = jnp.dot(same_tile, spread, preferred_element_type=jnp.float32)
        weights.append(flat.T.astype(jnp.bfloat16))

    tile_of_lane = iota((pair, 128), 1) // SHELL
    diagonal = iota((pair, 128), 0) % SHELL == iota((pair, 128), 1) % SHELL
    for g in range(groups):
        loads[g].wait()
        total = jnp.zeros((pair, 128), jnp.float32)
        for i in range(PACK):
            result = jnp.dot(tiles[g * PACK + i], weights[g], preferred_element_type=jnp.float32)
            total = jnp.where(tile_of_lane == i, result, total)
        total = jnp.where(diagonal, total, 0.0).reshape(SHELL, SHELL, 128)
        out_ref[pl.ds(g * SHELL, SHELL), :] = jnp.sum(total, axis=1)


def gather_kernel(colors, sizes, own_ref, all_ref, send_sem, recv_sem, local_sem):
    gx, gy, gz = lax.axis_index("gx"), lax.axis_index("gy"), lax.axis_index("gz")
    mine = {"c": lax.rem(gz, 2), "x": lax.div(gz, 2), "y": gx, "z": gy}
    dims = ("c", "x", "y", "z")

    def device(where):
        return {"gx": where["y"], "gy": where["z"], "gz": where["x"] * 2 + where["c"]}

    def peer(dim, step):
        return device(dict(mine, **{dim: lax.rem(mine[dim] + step, sizes[dim])}))

    barrier = pltpu.get_barrier_semaphore()
    greeted = 0
    for dim in dims:
        for step in range(1, sizes[dim]):
            pl.semaphore_signal(barrier, inc=1, device_id=peer(dim, step), device_id_type=MESH)
            greeted += 1
    pl.semaphore_wait(barrier, greeted)

    here = pltpu.make_async_copy(
        own_ref, all_ref.at[mine["c"], mine["x"], mine["y"], mine["z"]], local_sem)
    here.start()

    pending = [[] for _ in colors]
    slot = 0
    for stage in range(len(dims)):
        for number, (first, rows, order) in enumerate(colors):
            for copy in pending[number]:
                copy.wait()
            pending[number] = []
            if stage == 1 and number == 0:
                here.wait()
            dim, done = order[stage], order[:stage]
            part = pl.ds(first, rows)
            index = tuple(pl.ds(0, sizes[d]) if d in done else mine[d] for d in dims)
            held = all_ref.at[index + (part,)]
            for step in range(1, sizes[dim]):
                copy = pltpu.make_async_remote_copy(
                    src_ref=own_ref.at[part] if stage == 0 else held, dst_ref=held,
                    send_sem=send_sem.at[slot], recv_sem=recv_sem.at[slot],
                    device_id=peer(dim, step), device_id_type=MESH)
                copy.start()
                pending[number].append(copy)
                slot += 1
    for copies in pending:
        for copy in copies:
            copy.wait()


def scatter_kernel(ket_bits, row_bits, row_shells, col_shells, width, all_ref, out_ref,
                   orders, order_smem, order_sem, out_sem, *slabs):
    cores, xs, ys, zs = all_ref.shape[:4]
    groups = all_ref.shape[4] // SHELL
    slab_rows = row_shells * SHELL
    code = all_ref[:, :, :, :, groups * SHELL, :].reshape(cores * xs * ys * zs, 128).astype(jnp.int32)
    ket = (code & ((1 << ket_bits) - 1)) - lax.axis_index("gy") * col_shells
    row = (code >> ket_bits) & ((1 << row_bits) - 1)
    owner = code >> (ket_bits + row_bits)
    valid = (owner == lax.axis_index("gx")) & (ket >= 0) & (ket < col_shells)
    orders[...] = jnp.where(valid, (row << ket_bits) + ket, row_shells << ket_bits)
    fetch = pltpu.make_async_copy(orders, order_smem, order_sem)
    fetch.start()

    def clear(shell, carry):
        for slab in slabs:
            slab[pl.ds(pl.multiple_of(shell * SHELL, SHELL), SHELL), :] = jnp.zeros((SHELL, width), jnp.float32)
        return carry

    lax.fori_loop(0, row_shells, clear, 0)
    fetch.wait()
    block_lane = iota((SHELL, 128), 1) // SHELL

    def add(step, carry):
        source, group = step // groups, step % groups
        y, z = source // zs, source % zs
        first = pl.multiple_of(group * SHELL, SHELL)
        values = [all_ref[s % 2, s // 2, y, z, pl.ds(first, SHELL), :] for s in range(len(slabs))]
        for i in range(PACK):
            for s, slab in enumerate(slabs):
                line = ((s % 2) * xs + s // 2) * ys * zs + source
                order = order_smem[line, group * PACK + i]
                shell = order >> ket_bits
                local = order & ((1 << ket_bits) - 1)
                spot = local & (PACK - 1)
                moved = pltpu.roll(values[s], ((spot - i) * SHELL) & 127, 1)
                moved = jnp.where(block_lane == spot, moved, 0.0)
                rows = pl.ds(pl.multiple_of(shell * SHELL, SHELL), SHELL)
                cols = pl.ds(pl.multiple_of((local // PACK) * 128, 128), 128)
                slab[rows, cols] = slab[rows, cols] + moved
        return carry

    lax.fori_loop(0, ys * zs * groups, add, 0)
    stores = []
    for s, slab in enumerate(slabs):
        store = pltpu.make_async_copy(slab.at[pl.ds(0, slab_rows), :],
                                      out_ref.at[pl.ds(s * slab_rows, slab_rows), :], out_sem.at[s])
        store.start()
        stores.append(store)
    for store in stores:
        store.wait()


def color_rows(rows):
    units = rows // 8
    first = max(1, units // 9)
    second = max(1, (units - first) * 3 // 8)
    third = units - first - second
    return [(0, first * 8, "xyzc"), (first * 8, second * 8, "yzxc"), ((first + second) * 8, third * 8, "zxyc")]


def solution(mesh):
    n_gx, n_gy, n_gz = mesh.shape["gx"], mesh.shape["gy"], mesh.shape["gz"]

    def shards(eri, owner, quartet, significance, density):
        tiles, pair = eri.shape[0], eri.shape[1]
        shells = density.shape[1] // SHELL
        row_shells, col_shells = shells // (n_gx * n_gz), shells // n_gy
        ket_bits, row_bits = (shells - 1).bit_length(), (row_shells - 1).bit_length()
        rows = tiles // PACK * SHELL + 8
        smem, hbm = pl.BlockSpec(memory_space=pltpu.SMEM), pl.BlockSpec(memory_space=pl.ANY)
        vmem = pl.BlockSpec(memory_space=pltpu.VMEM)
        limit = 48 * 1024 * 1024
        own = pl.pallas_call(
            functools.partial(contract_kernel, ket_bits, row_bits),
            out_shape=jax.ShapeDtypeStruct((rows, 128), jnp.float32),
            in_specs=[smem, smem, smem, hbm, hbm],
            out_specs=vmem,
            scratch_shapes=[
                pltpu.VMEM(eri.shape, jnp.bfloat16),
                pltpu.VMEM((tiles * SHELL, 128), jnp.bfloat16),
                pltpu.VMEM((tiles * SHELL, 128), jnp.bfloat16),
                pltpu.SemaphoreType.DMA((tiles // PACK,)),
                pltpu.SemaphoreType.DMA((tiles,)),
            ],
            compiler_params=pltpu.CompilerParams(vmem_limit_bytes=limit),
            name="contract",
        )(owner, quartet, significance, eri, density)

        sizes = {"c": 2, "x": n_gz // 2, "y": n_gx, "z": n_gy}
        colors = color_rows(rows)
        slots = len(colors) * sum(size - 1 for size in sizes.values())
        everyone = pl.pallas_call(
            functools.partial(gather_kernel, colors, sizes),
            out_shape=jax.ShapeDtypeStruct((2, n_gz // 2, n_gx, n_gy, rows, 128), jnp.float32),
            in_specs=[vmem],
            out_specs=vmem,
            scratch_shapes=[
                pltpu.SemaphoreType.DMA((slots,)),
                pltpu.SemaphoreType.DMA((slots,)),
                pltpu.SemaphoreType.DMA,
            ],
            compiler_params=pltpu.CompilerParams(
                collective_id=0, has_side_effects=True, vmem_limit_bytes=limit),
            name="gather",
        )(own)

        width = -(-col_shells * SHELL // 128) * 128
        devices = n_gx * n_gy * n_gz
        out = pl.pallas_call(
            functools.partial(scatter_kernel, ket_bits, row_bits, row_shells, col_shells, width),
            out_shape=jax.ShapeDtypeStruct((n_gz * row_shells * SHELL, width), jnp.float32),
            in_specs=[vmem],
            out_specs=hbm,
            scratch_shapes=[
                pltpu.VMEM((devices, 128), jnp.int32),
                pltpu.SMEM((devices, 128), jnp.int32),
                pltpu.SemaphoreType.DMA,
                pltpu.SemaphoreType.DMA((n_gz,)),
            ] + [pltpu.VMEM(((row_shells + 1) * SHELL, width), jnp.float32)] * n_gz,
            compiler_params=pltpu.CompilerParams(vmem_limit_bytes=limit),
            name="scatter",
        )(everyone)
        return out if width == col_shells * SHELL else out[:, :col_shells * SHELL]

    in_specs = (
        P(("gx", "gy", "gz"), None, None),
        P(("gx", "gy", "gz"), None),
        P(("gx", "gy", "gz"), None),
        P(("gx", "gy", "gz")),
        P("gy", None),
    )
    return jax.shard_map(shards, mesh=mesh, in_specs=in_specs, out_specs=P("gx", "gy"), check_vma=False)
```

```python
import functools

import jax
import jax.numpy as jnp
from jax import lax
from jax.experimental import pallas as pl
from jax.experimental.pallas import tpu as pltpu
from jax.sharding import PartitionSpec as P

SHELL = 16
PACK = 128 // SHELL
MESH = pl.DeviceIdType.MESH


def iota(shape, dim):
    return lax.broadcasted_iota(jnp.int32, shape, dim)


def contract_kernel(ket_bits, row_bits, owner_ref, quartet_ref, keep_ref, eri_ref, density_ref,
                    out_ref, tiles, picked, masked, tile_sem, pick_sem):
    count = eri_ref.shape[0]
    groups = count // PACK
    picks = []
    for t in range(count):
        row = pl.multiple_of(quartet_ref[2, t] * SHELL, SHELL)
        col = pl.multiple_of((quartet_ref[3, t] // PACK) * 128, 128)
        pick = pltpu.make_async_copy(density_ref.at[pl.ds(row, SHELL), pl.ds(col, 128)],
                                     picked.at[pl.ds(t * SHELL, SHELL), :], pick_sem.at[t])
        pick.start()
        picks.append(pick)
    loads = []
    for g in range(groups):
        part = pl.ds(g * PACK, PACK)
        load = pltpu.make_async_copy(eri_ref.at[part], tiles.at[part], tile_sem.at[g])
        load.start()
        loads.append(load)

    lane = iota((8, 128), 1)
    codes = jnp.zeros((8, 128), jnp.int32)
    for t in range(count):
        code = (owner_ref[0, t] << (ket_bits + row_bits)) + (quartet_ref[0, t] << ket_bits) + quartet_ref[1, t]
        codes = jnp.where(lane == t, code, codes)
    out_ref[pl.ds(groups * SHELL, 8), :] = codes.astype(jnp.float32)

    block_lane = iota((SHELL, 128), 1) // SHELL
    for t in range(count):
        picks[t].wait()
        place = jnp.where(keep_ref[t] > 0, lax.rem(quartet_ref[3, t], PACK), -1)
        rows = pl.ds(t * SHELL, SHELL)
        block = picked[rows, :].astype(jnp.float32)
        masked[rows, :] = jnp.where(block_lane == place, block, 0.0).astype(jnp.bfloat16)

    pair = SHELL * SHELL
    repeat = (iota((128, pair), 0) % SHELL == iota((128, pair), 1) % SHELL).astype(jnp.bfloat16)
    own_row = iota((128, pair), 0) % SHELL == iota((128, pair), 1) // SHELL
    same_tile = (iota((128, 128), 0) // SHELL == iota((128, 128), 1) // SHELL).astype(jnp.bfloat16)
    weights = []
    for g in range(groups):
        spread = jnp.dot(masked[pl.ds(g * 128, 128), :], repeat, preferred_element_type=jnp.float32)
        spread = jnp.where(own_row, spread, 0.0).astype(jnp.bfloat16)
        flat = jnp.dot(same_tile, spread, preferred_element_type=jnp.float32)
        weights.append(flat.T.astype(jnp.bfloat16))

    tile_of_lane = iota((pair, 128), 1) // SHELL
    diagonal = iota((pair, 128), 0) % SHELL == iota((pair, 128), 1) % SHELL
    for g in range(groups):
        loads[g].wait()
        total = jnp.zeros((pair, 128), jnp.float32)
        for i in range(PACK):
            result = jnp.dot(tiles[g * PACK + i], weights[g], preferred_element_type=jnp.float32)
            total = jnp.where(tile_of_lane == i, result, total)
        total = jnp.where(diagonal, total, 0.0).reshape(SHELL, SHELL, 128)
        out_ref[pl.ds(g * SHELL, SHELL), :] = jnp.sum(total, axis=1)


def other(index, step, size):
    if size & (size - 1):
        return lax.rem(index + step, size)
    bit = 1
    while bit <= step:
        if step & bit:
            index = index + bit - 2 * bit * lax.rem(lax.div(index, bit), 2)
        bit *= 2
    return index


def source_of(index, step, size):
    return lax.rem(index + size - step, size) if size & (size - 1) else other(index, step, size)


def gather_kernel(sizes, own_ref, all_ref, send_sem, recv_sem, local_sem):
    gx, gy, gz = lax.axis_index("gx"), lax.axis_index("gy"), lax.axis_index("gz")
    core, x, y, z = lax.rem(gz, 2), lax.div(gz, 2), gx, gy
    xs, ys, zs = sizes

    def device(core, x, y, z):
        return {"gx": y, "gy": z, "gz": x * 2 + core}

    plane = [(dx, dy) for dx in range(xs) for dy in range(ys) if dx or dy]
    plane.sort(key=lambda step: (-(step[0] > 0) - (step[1] > 0), step))
    flat = {step: device(core, other(x, step[0], xs), other(y, step[1], ys), z) for step in plane}
    column = {step: device(core, x, y, other(z, step, zs)) for step in range(1, zs)}
    twin = device(1 - core, x, y, z)

    barrier = pltpu.get_barrier_semaphore()
    peers = list(flat.values()) + list(column.values()) + [twin]
    for peer in peers:
        pl.semaphore_signal(barrier, inc=1, device_id=peer, device_id_type=MESH)
    pl.semaphore_wait(barrier, len(peers))

    slots = iter(range(send_sem.shape[0]))

    def send(source, place, peer):
        slot = next(slots)
        copy = pltpu.make_async_remote_copy(
            src_ref=source, dst_ref=all_ref.at[place], send_sem=send_sem.at[slot],
            recv_sem=recv_sem.at[slot], device_id=peer, device_id_type=MESH)
        copy.start()
        return copy

    here = pltpu.make_async_copy(own_ref, all_ref.at[core, x, y, z], local_sem)
    here.start()
    sent, arrivals = [], []

    def spread(source, place):
        for step in plane:
            arrivals.append((send(source, place, flat[step]), step, place[3]))
        sent.append(send(source, place, twin))

    place = (core, x, y, z)
    steps = [send(own_ref, place, column[step]) for step in range(1, zs)]
    spread(own_ref, place)
    for step, copy in enumerate(steps, 1):
        copy.wait_recv()
        place = (core, x, y, source_of(z, step, zs))
        spread(all_ref.at[place], place)
    for copy, (dx, dy), depth in arrivals:
        copy.wait_recv()
        place = (core, source_of(x, dx, xs), source_of(y, dy, ys), depth)
        sent.append(send(all_ref.at[place], place, twin))
    for copy in sent:
        copy.wait_recv()
    for copy in steps + [copy for copy, _, _ in arrivals] + sent:
        copy.wait_send()
    here.wait()


def scatter_kernel(ket_bits, row_bits, row_shells, col_shells, width, all_ref, out_ref,
                   table, table_smem, table_sem, out_sem, *slabs):
    cores, xs, ys, zs = all_ref.shape[:4]
    groups = all_ref.shape[4] // SHELL
    lines = cores * xs * ys * zs
    slab_rows = row_shells * SHELL
    tall = slab_rows + SHELL
    code = all_ref[:, :, :, :, groups * SHELL, :].reshape(lines, 128).astype(jnp.int32)
    ket = (code & ((1 << ket_bits) - 1)) - lax.axis_index("gy") * col_shells
    row = (code >> ket_bits) & ((1 << row_bits) - 1)
    owner = code >> (ket_bits + row_bits)
    valid = (owner == lax.axis_index("gx")) & (ket >= 0) & (ket < col_shells)
    spot = (ket // PACK) * tall + row * SHELL
    table[pl.ds(0, lines), :] = jnp.where(valid, spot, slab_rows)
    table[pl.ds(lines, lines), :] = ((ket - iota((lines, 128), 1)) * SHELL) & 127
    fetch = pltpu.make_async_copy(table, table_smem, table_sem)
    fetch.start()

    def clear(shell, carry):
        rows = pl.ds(pl.multiple_of(shell * 2 * SHELL, SHELL), 2 * SHELL)
        for slab in slabs:
            slab[rows, :] = jnp.zeros((2 * SHELL, 128), jnp.float32)
        return carry

    lax.fori_loop(0, slabs[0].shape[0] // (2 * SHELL), clear, 0)
    fetch.wait()
    block_lane = iota((SHELL, 128), 1) // SHELL

    def add(step, carry):
        source, group = step // groups, step % groups
        y, z = source // zs, source % zs
        first = pl.multiple_of(group * SHELL, SHELL)
        values = [all_ref[s % 2, s // 2, y, z, pl.ds(first, SHELL), :] for s in range(len(slabs))]
        for i in range(PACK):
            for s, slab in enumerate(slabs):
                line = ((s % 2) * xs + s // 2) * ys * zs + source
                lane = group * PACK + i
                moved = pltpu.roll(jnp.where(block_lane == i, values[s], 0.0), table_smem[lines + line, lane], 1)
                rows = pl.ds(pl.multiple_of(table_smem[line, lane], SHELL), SHELL)
                slab[rows, :] = slab[rows, :] + moved
        return carry

    lax.fori_loop(0, ys * zs * groups, add, 0)
    stores = []
    for s, slab in enumerate(slabs):
        for block in range(width // 128):
            store = pltpu.make_async_copy(
                slab.at[pl.ds(block * tall, slab_rows), :],
                out_ref.at[pl.ds(s * slab_rows, slab_rows), pl.ds(block * 128, 128)],
                out_sem.at[s, block])
            store.start()
            stores.append(store)
    for store in stores:
        store.wait()


def solution(mesh):
    n_gx, n_gy, n_gz = mesh.shape["gx"], mesh.shape["gy"], mesh.shape["gz"]

    def shards(eri, owner, quartet, significance, density):
        tiles, pair = eri.shape[0], eri.shape[1]
        shells = density.shape[1] // SHELL
        row_shells, col_shells = shells // (n_gx * n_gz), shells // n_gy
        ket_bits, row_bits = (shells - 1).bit_length(), (row_shells - 1).bit_length()
        rows = tiles // PACK * SHELL + 8
        smem, hbm = pl.BlockSpec(memory_space=pltpu.SMEM), pl.BlockSpec(memory_space=pl.ANY)
        vmem = pl.BlockSpec(memory_space=pltpu.VMEM)
        limit = 48 * 1024 * 1024
        own = pl.pallas_call(
            functools.partial(contract_kernel, ket_bits, row_bits),
            out_shape=jax.ShapeDtypeStruct((rows, 128), jnp.float32),
            in_specs=[smem, smem, smem, pl.BlockSpec(memory_space=pltpu.HBM), hbm],
            out_specs=vmem,
            scratch_shapes=[
                pltpu.VMEM(eri.shape, jnp.bfloat16),
                pltpu.VMEM((tiles * SHELL, 128), jnp.bfloat16),
                pltpu.VMEM((tiles * SHELL, 128), jnp.bfloat16),
                pltpu.SemaphoreType.DMA((tiles // PACK,)),
                pltpu.SemaphoreType.DMA((tiles,)),
            ],
            compiler_params=pltpu.CompilerParams(vmem_limit_bytes=60 * 1024 * 1024),
            name="contract",
        )(owner.T, quartet.T, significance, eri, density)

        sizes = (n_gz // 2, n_gx, n_gy)
        plane = sizes[0] * sizes[1]
        slots = n_gy - 1 + n_gy * (plane - 1) + n_gy * plane
        everyone = pl.pallas_call(
            functools.partial(gather_kernel, sizes),
            out_shape=jax.ShapeDtypeStruct((2, n_gz // 2, n_gx, n_gy, rows, 128), jnp.float32),
            in_specs=[vmem],
            out_specs=vmem,
            scratch_shapes=[
                pltpu.SemaphoreType.DMA((slots,)),
                pltpu.SemaphoreType.DMA((slots,)),
                pltpu.SemaphoreType.DMA,
            ],
            compiler_params=pltpu.CompilerParams(
                collective_id=0, has_side_effects=True, vmem_limit_bytes=limit),
            name="gather",
        )(own)

        width = -(-col_shells * SHELL // 128) * 128
        devices = n_gx * n_gy * n_gz
        out = pl.pallas_call(
            functools.partial(scatter_kernel, ket_bits, row_bits, row_shells, col_shells, width),
            out_shape=jax.ShapeDtypeStruct((n_gz * row_shells * SHELL, width), jnp.float32),
            in_specs=[vmem],
            out_specs=hbm,
            scratch_shapes=[
                pltpu.VMEM((2 * devices, 128), jnp.int32),
                pltpu.SMEM((2 * devices, 128), jnp.int32),
                pltpu.SemaphoreType.DMA,
                pltpu.SemaphoreType.DMA((n_gz, width // 128)),
            ] + [pltpu.VMEM((-(-(row_shells + 1) * (width // 128) // 2) * 2 * SHELL, 128), jnp.float32)] * n_gz,
            compiler_params=pltpu.CompilerParams(vmem_limit_bytes=limit),
            name="scatter",
        )(everyone)
        return out if width == col_shells * SHELL else out[:, :col_shells * SHELL]

    in_specs = (
        P(("gx", "gy", "gz"), None, None),
        P(("gx", "gy", "gz"), None),
        P(("gx", "gy", "gz"), None),
        P(("gx", "gy", "gz")),
        P("gy", None),
    )
    return jax.shard_map(shards, mesh=mesh, in_specs=in_specs, out_specs=P("gx", "gy"), check_vma=False)
```
